32 devices in a mesh: trial: 4 (over y, x), rows: 4 (over z), cols: 2 (over core).
Axes of the slice: x: 2, y: 2, z: 4, core: 2. Of those that a mesh axis runs over, the one named last changes fastest.
Arguments:
- weight_query: bfloat16 [20480, 5120], P(('trial', 'rows'), 'cols'), parts along dimension 0, may hold values from -0.078125 to 0.078125
- low_query: bfloat16 [20480, 32], P(('trial', 'rows')), parts along dimension 0, may hold values from -0.078125 to 0.078125
- high_query: bfloat16 [128, 5120], P('trial', 'cols'), parts along dimension 0, may hold values from -1 to 1
- weight_key: bfloat16 [20480, 1024], P(('trial', 'rows'), 'cols'), parts along dimension 0, may hold values from -0.078125 to 0.078125
- low_key: bfloat16 [20480, 32], P(('trial', 'rows')), parts along dimension 0, may hold values from -0.078125 to 0.078125
- high_key: bfloat16 [128, 1024], P('trial', 'cols'), parts along dimension 0, may hold values from -1 to 1
- weight_value: bfloat16 [20480, 1024], P(('trial', 'rows'), 'cols'), parts along dimension 0, may hold values from -0.078125 to 0.078125
- low_value: bfloat16 [20480, 32], P(('trial', 'rows')), parts along dimension 0, may hold values from -0.078125 to 0.078125
- high_value: bfloat16 [128, 1024], P('trial', 'cols'), parts along dimension 0, may hold values from -1 to 1
- norm_train: float32 [20480], P(('trial', 'rows', 'cols')), parts along dimension 0, may hold values from 0.25 to 1.75
- norm_step: float32 [20480], P(('trial', 'rows', 'cols')), parts along dimension 0, may hold values from -0.3 to 0.3
Outputs:
- serve_query: bfloat16 [20480, 5120], P(('trial', 'cols')), parts along dimension 0
- serve_key: bfloat16 [4096, 5120], P(('trial', 'cols')), parts along dimension 0
- serve_value: bfloat16 [4096, 5120], P(('trial', 'cols')), parts along dimension 0
- serve_norm: bfloat16 [20480], P('trial'), parts along dimension 0
The draws below stay inside these ranges and needn't reach their ends.
There are 4 independent parts, one for each index of `trial`. The reference program is written for one: setup_inputs(seed, part) draws one part's arguments, and reference() takes and returns one part's arrays. A program takes and returns all parts, laid end to end along the dimension named above; each array names one. Nothing has to cross between parts.
All inputs are finite; a program needn't handle non-finite values.
Results may differ from the reference program's by a relative error of at most 0.001.
Values may be sent and summed in bfloat16 or wider, within the bound.
A program may use at most 128 MiB of HBM per device.

```python
import jax
import jax.numpy as jnp

D_MODEL = 5120
Q_DIM = 5120
KV_DIM = 1024
RANK = 32


def levels(own_key, shape, cuts, low, top_value):
    factor_of = 1.0
    for dim, shards_of in cuts:
        steps = jax.random.uniform(jax.random.fold_in(jax.random.fold_in(own_key, 6), dim), (shards_of,), jnp.float32, low / len(cuts), top_value / len(cuts))
        factor_of = factor_of * jnp.repeat(jnp.exp(steps), shape[dim] // shards_of).reshape((-1,) + (1,) * (len(shape) - 1 - dim))
    return factor_of


def gaussian(own_key, dims, width, limit, split=(), dtype=jnp.bfloat16):
    entries = jax.random.normal(own_key, dims, jnp.float32) * width
    if len(split) > 0:
        entries = levels(own_key, dims, split, -0.22, 0.18) * entries
    return jnp.clip(entries, min=-limit, max=limit).astype(dtype)


def setup_inputs(seed: int = 0, part: int = 0) -> dict:
    key_of = jax.random.split(jax.random.key(seed), 12)
    own_keys = jax.random.split(jax.random.fold_in(key_of[11], part), 12)
    return {
        "weight_query": gaussian(own_keys[0], (D_MODEL, Q_DIM), D_MODEL ** -0.5, 0.078125, ((0, 4), (1, 2))),
        "low_query": gaussian(own_keys[1], (D_MODEL, RANK), D_MODEL ** -0.5, 0.078125, ((0, 4),)),
        "high_query": gaussian(own_keys[2], (RANK, Q_DIM), RANK ** -0.5, 1.0, ((1, 2),)),
        "weight_key": gaussian(own_keys[3], (D_MODEL, KV_DIM), D_MODEL ** -0.5, 0.078125, ((0, 4), (1, 2))),
        "low_key": gaussian(own_keys[4], (D_MODEL, RANK), D_MODEL ** -0.5, 0.078125, ((0, 4),)),
        "high_key": gaussian(own_keys[5], (RANK, KV_DIM), RANK ** -0.5, 1.0, ((1, 2),)),
        "weight_value": gaussian(own_keys[6], (D_MODEL, KV_DIM), D_MODEL ** -0.5, 0.078125, ((0, 4), (1, 2))),
        "low_value": gaussian(own_keys[7], (D_MODEL, RANK), D_MODEL ** -0.5, 0.078125, ((0, 4),)),
        "high_value": gaussian(own_keys[8], (RANK, KV_DIM), RANK ** -0.5, 1.0, ((1, 2),)),
        "norm_train": jnp.clip(1.0 + 0.15 * jax.random.normal(own_keys[9], (D_MODEL,), jnp.float32), 0.25, 1.75),
        "norm_step": jnp.clip(jax.random.uniform(own_keys[10], (D_MODEL,), jnp.float32, -0.3, 0.3) * levels(own_keys[10], (D_MODEL,), ((0, 8),), -0.4, 0.0), -0.3, 0.3),
    }


mix_rate = 2.0


def reference(weight_query, low_query, high_query, weight_key, low_key, high_key, weight_value, low_value, high_value, norm_train, norm_step):
    fresh_query = weight_query.astype(jnp.float32) + mix_rate * jnp.dot(low_query, high_query, preferred_element_type=jnp.float32)
    fresh_key = weight_key.astype(jnp.float32) + mix_rate * jnp.dot(low_key, high_key, preferred_element_type=jnp.float32)
    fresh_value = weight_value.astype(jnp.float32) + mix_rate * jnp.dot(low_value, high_value, preferred_element_type=jnp.float32)
    serve_query = fresh_query.T.astype(jnp.bfloat16)
    serve_key = fresh_key.T.astype(jnp.bfloat16)
    serve_value = fresh_value.T.astype(jnp.bfloat16)
    serve_norm = (norm_train + norm_step).astype(jnp.bfloat16)
    return serve_query, serve_key, serve_value, serve_norm
```

```python
import functools

import jax
import jax.numpy as jnp
from jax import lax
from jax.experimental import pallas as pl
from jax.experimental.pallas import tpu as pltpu
from jax.sharding import PartitionSpec as P

mix_rate = 2.0


def merge_kernel(weight, low, high, out):
    product = lax.dot_general(
        high[...], low[...], (((0,), (0,)), ((), ())), preferred_element_type=jnp.float32
    )
    turned = weight[...].astype(jnp.float32).T
    out[...] = (turned + mix_rate * product).astype(jnp.bfloat16)


def merge(weight, low, high, first, size):
    depth, rank = low.shape
    step = 256 if size % 256 == 0 and first % 256 == 0 else 128
    base = first // step
    return pl.pallas_call(
        merge_kernel,
        grid=(size // step,),
        in_specs=[
            pl.BlockSpec((depth, step), lambda i: (0, base + i)),
            pl.BlockSpec((rank, depth), lambda i: (0, 0)),
            pl.BlockSpec((rank, step), lambda i: (0, base + i)),
        ],
        out_specs=pl.BlockSpec((step, depth), lambda i: (i, 0)),
        out_shape=jax.ShapeDtypeStruct((size, depth), jnp.bfloat16),
        cost_estimate=pl.CostEstimate(
            flops=2 * size * depth * rank, bytes_accessed=4 * size * depth, transcendentals=0
        ),
    )(weight, low.T, high)


def place_kernel(ways, first, hops, *refs):
    reach = len(hops)
    sources, (out, held, in_sem, out_sem) = refs[: 2 * reach], refs[-4:]
    me = lax.axis_index("rows")
    size, depth = held.shape[1:]
    pieces = []
    for up, down, hop in zip(sources[:reach], sources[reach:], hops):
        pieces.append((up, hop, me - hop, me >= hop))
        if hop > 0:
            pieces.append((down, ways - hop, me + hop, me + hop < ways))

    def fetch(piece):
        source, slot, _, _ = piece
        return pltpu.make_async_copy(source.at[pl.ds(0, size)], held.at[slot], in_sem.at[slot])

    def store(piece):
        _, slot, owner, _ = piece
        columns = pl.ds(pl.multiple_of(owner * depth, 128), depth)
        return pltpu.make_async_copy(
            held.at[slot], out.at[pl.ds(first, size), columns], out_sem.at[slot]
        )

    def hand_over(piece):
        fetch(piece).wait()
        store(piece).start()

    for piece in pieces:
        pl.when(piece[3])(lambda piece=piece: fetch(piece).start())
    for piece in pieces:
        pl.when(piece[3])(functools.partial(hand_over, piece))
    for piece in pieces:
        pl.when(piece[3])(lambda piece=piece: store(piece).wait())


def place(ways, ups, downs, hops, result, first, size, total):
    depth = ups[0].shape[1]
    arrays = [ups[hop] for hop in hops] + [downs[hop] for hop in hops]
    arrays += [] if result is None else [result]
    return pl.pallas_call(
        functools.partial(place_kernel, ways, first, hops),
        in_specs=[pl.BlockSpec(memory_space=pl.ANY)] * len(arrays),
        out_specs=pl.BlockSpec(memory_space=pl.ANY),
        out_shape=jax.ShapeDtypeStruct((total, ways * depth), jnp.bfloat16),
        scratch_shapes=[
            pltpu.VMEM((ways, size, depth), jnp.bfloat16),
            pltpu.SemaphoreType.DMA((ways,)),
            pltpu.SemaphoreType.DMA((ways,)),
        ],
        input_output_aliases={} if result is None else {len(arrays) - 1: 0},
        cost_estimate=pl.CostEstimate(
            flops=0, bytes_accessed=4 * size * depth * len(hops), transcendentals=0
        ),
    )(*arrays)


def after(array, other):
    return lax.optimization_barrier((array, other))[0]


def cuts(total, most):
    size = total
    while size > most and size % 256 == 0:
        size //= 2
    if size > most or total % 5 == 0 and total > 5 * 128:
        size = total // 5
    return [(first, size) for first in range(0, total, size)]


def local(ways, sides, wq, lq, hq, wk, lk, hk, wv, lv, hv, norm_train, norm_step):
    chunks = [
        (name, first, size)
        for name, array in (("key", wk), ("query", wq), ("value", wv))
        for first, size in cuts(array.shape[1], 512)
    ]
    tensors = {"query": (wq, lq, hq), "key": (wk, lk, hk), "value": (wv, lv, hv)}
    ups = []
    for name, first, size in chunks:
        weight, low, high = tensors[name]
        ups.append([merge(weight, low, high, first, size)])
    carrier = 1
    mine = (norm_train + norm_step).astype(jnp.bfloat16).reshape(1, -1)
    width = wq.shape[0]
    ups[carrier][0] = jnp.concatenate(
        [ups[carrier][0], jnp.broadcast_to(jnp.tile(mine, (1, sides)), (8, width))], axis=0
    )
    downs = [list(up) for up in ups]
    for hop in range(1, ways):
        for index, (up, down) in enumerate(zip(ups, downs)):
            rising, falling = up[-1], down[-1]
            up.append(
                lax.ppermute(rising, "rows", [(i, i + 1) for i in range(hop - 1, ways - 1)])
            )
            down.append(
                lax.ppermute(falling, "rows", [(i, i - 1) for i in range(1, ways - hop + 1)])
            )
    results = {"query": None, "key": None, "value": None}
    for index, (name, first, size) in enumerate(chunks):
        groups = [tuple(range(ways))]
        if index == len(chunks) - 1:
            groups = [tuple(range(ways - 1)), (ways - 1,)]
        for hops in groups:
            if hops[0] > 0:
                ups[index][-1] = after(ups[index][-1], results["query"])
            results[name] = place(
                ways, ups[index], downs[index], hops, results[name], first, size,
                tensors[name][0].shape[1],
            )
    me, side = lax.axis_index("rows"), lax.axis_index("cols")
    size, share = chunks[carrier][2], mine.shape[1]
    rounds = [mine]
    for hop in range(1, ways):
        up, down = ups[carrier][hop], downs[carrier][ways - hop]
        rounds.append(jnp.where(me >= hop, up[size : size + 1, :share], down[size : size + 1, :share]))
    order = lax.rem(me - jnp.arange(ways) + ways, ways)
    held = jnp.take(jnp.concatenate(rounds), order, axis=0)
    parts = [held]
    for step in range(1, sides):
        pairs = [(i, (i + step) % sides) for i in range(sides)]
        parts.append(lax.ppermute(held, "cols", pairs))
    order = lax.rem(side - jnp.arange(sides) + sides, sides)
    serve_norm = jnp.take(jnp.stack(parts, axis=1), order, axis=1).reshape(-1)
    return (results["query"], results["key"], results["value"], serve_norm)


def solution(mesh):
    return jax.shard_map(
        functools.partial(local, mesh.shape["rows"], mesh.shape["cols"]),
        mesh=mesh,
        in_specs=(
            P(("trial", "rows"), "cols"),
            P(("trial", "rows"), None),
            P("trial", "cols"),
            P(("trial", "rows"), "cols"),
            P(("trial", "rows"), None),
            P("trial", "cols"),
            P(("trial", "rows"), "cols"),
            P(("trial", "rows"), None),
            P("trial", "cols"),
            P(("trial", "rows", "cols")),
            P(("trial", "rows", "cols")),
        ),
        out_specs=(
            P(("trial", "cols"), None),
            P(("trial", "cols"), None),
            P(("trial", "cols"), None),
            P("trial"),
        ),
        check_vma=False,
    )
```
